32 devices in a mesh: grp: 4 (over y, x), shard: 8 (over z, core).
Axes of the slice: x: 2, y: 2, z: 4, core: 2. Of those that a mesh axis runs over, the one named last changes fastest.
Arguments:
- bottom_out: bfloat16 [4096, 128], P(('grp', 'shard')), may hold values from -6 to 6
- lookups: int32 [4096, 1, 4], P(('grp', 'shard')), may hold values from 0 to 62975, as said below
- starts: int32 [4, 32], replicated, may hold values from 0 to 1967
- tables: float32 [1, 62976, 128], P(None, 'shard'), may hold values from -0.3 to 0.3
- top_dense: bfloat16 [128, 1024], replicated, may hold values from -0.5 to 0.5
- top_pairs: float32 [1, 1024], replicated, may hold values from -6 to 6
- cotangent: float32 [4096, 1024], P(('grp', 'shard')), may hold values from -1.5 to 1.5
Outputs:
- activation: bfloat16 [4096, 1024], P(('grp', 'shard'))
- bottom_grad: float32 [4096, 128], P(('grp', 'shard'))
- table_grad: float32 [1, 8, 7872, 128], P(None, 'shard', 'grp')
The draws below stay inside these ranges and needn't reach their ends.
Inputs may be any that keep to these rules, and one draw needn't show every extreme that they name: lookups % 1968 is below 64, and 63 occurs.
All inputs are finite; a program needn't handle non-finite values.
Results may differ from the reference program's by a relative error of at most 0.0023.
Values sent between devices are 32-bit elements; how exact they have to be, the bound alone decides.
A program may use at most 64 MiB of HBM per device.

```python
import jax
import jax.numpy as jnp
from jax import lax

D = 128
HIDDEN_SIZE = 1024
ROWS_DEV = 7872
NT = 1
BAG = 4
HOT = 64
B_DEV = 128
ROWS = 62976
WIN = 1968
WINDOWS = 32
BATCH = 4096
PAIRS = 1
N_GRP = 4
N_SHARD = 8


def draw_lookups(key, part):
    first_key = jax.random.fold_in(key, 11)
    second_key = jax.random.fold_in(key, 23)
    window = jax.random.randint(first_key, (BATCH, NT, BAG), 0, WINDOWS, dtype=jnp.int32)
    inner = jax.random.randint(second_key, (BATCH, NT, BAG), 0, HOT, dtype=jnp.int32)
    return (window * WIN + inner).astype(jnp.int32)


def touch_ends(values, stream_key, least, top_value):
    spot = [jax.random.randint(jax.random.fold_in(stream_key, axis), (), 0, length) for axis, length in enumerate(values.shape)]
    widest = values.shape.index(max(values.shape))
    next_to = spot[:widest] + [(spot[widest] + 1) % values.shape[widest]] + spot[widest + 1:]
    return values.at[tuple(spot)].set(least).at[tuple(next_to)].set(top_value)


def levels(key, shape, shards, low, largest):
    def one(position, shards_of):
        draws = jax.random.uniform(jax.random.fold_in(jax.random.fold_in(key, 6), position), (shards_of,), jnp.float32, low / len(shards), largest / len(shards))
        return jnp.repeat(jnp.exp(draws), shape[position] // shards_of).reshape((-1,) + (1,) * (len(shape) - position - 1))

    loudness = one(*shards[0])
    for cut in shards[1:]:
        loudness = loudness * one(*cut)
    return loudness


def normal_values(own_key, dims, spread, most, cuts=(), held_as=jnp.bfloat16):
    values = jax.random.normal(own_key, dims, jnp.float32) * spread
    if len(cuts) > 0:
        values = levels(own_key, dims, cuts, -0.22, 0.18) * values
    return jnp.clip(values, min=-most, max=most).astype(held_as)


def setup_inputs(seed: int = 0) -> dict:
    key_list = jax.random.split(jax.random.key(seed), 8)
    return {
        "bottom_out": normal_values(key_list[0], (BATCH, D), 1.0, 6.0, ((0, 32),)),
        "lookups": draw_lookups(jax.random.fold_in(key_list[7], 71), 0),
        "starts": touch_ends(jax.random.randint(key_list[2], (N_GRP, WINDOWS), 0, WIN), jax.random.fold_in(key_list[2], 1), 0, WIN - 1).astype(jnp.int32),
        "tables": normal_values(key_list[3], (NT, ROWS, D), 0.05, 0.3, ((1, 8),), jnp.float32),
        "top_dense": normal_values(key_list[4], (D, HIDDEN_SIZE), D ** -0.5, 0.5),
        "top_pairs": normal_values(key_list[5], (PAIRS, HIDDEN_SIZE), PAIRS ** -0.5, 6.0, (), jnp.float32),
        "cotangent": normal_values(key_list[6], (BATCH, HIDDEN_SIZE), 0.25, 1.5, ((0, 32),), jnp.float32),
    }


def pair_list(number):
    return [(former, latter) for former in range(number) for latter in range(former + 1, number)]


def reference(bottom_out, lookups, starts, tables, top_dense, top_pairs, cotangent):
    group_of = (jnp.arange(BATCH, dtype=jnp.int32) // (B_DEV * N_SHARD)).astype(jnp.int32)
    window = (lookups // WIN).astype(jnp.int32)
    inner = (lookups % WIN).astype(jnp.int32)
    shift = starts[group_of[:, None, None], window]
    rows = (window * WIN + (inner + shift) % WIN).astype(jnp.int32)
    pooled_list = []
    for table_pos in range(NT):
        running = jnp.zeros((BATCH, D), jnp.float32)
        for slot in range(BAG):
            running = running + tables[table_pos][rows[:, table_pos, slot]]
        pooled_list.append(running)
    vectors = [bottom_out.astype(jnp.float32)] + pooled_list
    couples = pair_list(NT + 1)
    pair_dots = jnp.stack([jnp.sum(vectors[former] * vectors[latter], axis=-1) for former, latter in couples], axis=1)
    preact = jnp.dot(bottom_out, top_dense, preferred_element_type=jnp.float32)
    preact = preact + jnp.dot(pair_dots, top_pairs, precision=lax.Precision.HIGHEST)
    sigmoid_pre = jax.nn.sigmoid(preact)
    activation = (preact * sigmoid_pre).astype(jnp.bfloat16)
    pre_grad = cotangent * sigmoid_pre * (1.0 + preact * (1.0 - sigmoid_pre))
    pair_grad = jnp.dot(pre_grad, top_pairs.T, precision=lax.Precision.HIGHEST)
    vec_grads = [jnp.zeros_like(vector) for vector in vectors]
    for place, (former, latter) in enumerate(couples):
        weight_col = pair_grad[:, place:place + 1]
        vec_grads[former] = vec_grads[former] + weight_col * vectors[latter]
        vec_grads[latter] = vec_grads[latter] + weight_col * vectors[former]
    pre_half = pre_grad.astype(jnp.bfloat16)
    bottom_grad = jnp.dot(pre_half, top_dense.T, preferred_element_type=jnp.float32) + vec_grads[0]
    grad_list = []
    for table_pos in range(NT):
        running = jnp.zeros((ROWS, D), jnp.float32)
        for slot in range(BAG):
            running = running.at[rows[:, table_pos, slot]].add(vec_grads[table_pos + 1])
        grad_list.append(running)
    table_grad = jnp.stack(grad_list, axis=0).reshape(NT, N_SHARD, ROWS_DEV, D)
    return activation, bottom_grad, table_grad
```

```python
import functools

import jax
import jax.numpy as jnp
from jax import lax
from jax.experimental import pallas as pl
from jax.experimental.pallas import tpu as pltpu
from jax.sharding import PartitionSpec as P

HOT = 64
MESH = pl.DeviceIdType.MESH
VMEM = pltpu.VMEM
DMA = pltpu.SemaphoreType.DMA


def split_two(value):
    high = value.astype(jnp.bfloat16)
    low = (value - high.astype(jnp.float32)).astype(jnp.bfloat16)
    return high, low


def exchange_kernel(
    groups, shards, window,
    starts_ref, lookups_ref, bottom_ref, tables_ref, dense_ref, pairs_ref, cot_ref,
    act_ref, bottom_grad_ref, hot_out_ref,
    tab, looks, bottoms, counts, part_far, part_own, from_sib, arrived, pair_all,
    weighted, preact_ref, half_ref, grad_send, grad_recv,
    tab_sem, look_send, look_recv, bot_send, bot_recv, sib_send, sib_recv,
    sum_send, sum_recv, pair_send, pair_recv, grp_send, grp_recv,
):
    bag, batch = lookups_ref.shape
    width = bottom_ref.shape[1]
    hidden = cot_ref.shape[1]
    chips = shards // 2
    hot_rows = groups * HOT
    me = lax.axis_index("shard")
    grp = lax.axis_index("grp")
    core = lax.rem(me, 2)
    chip = lax.div(me, 2)
    sib = chip * 2 + 1 - core

    def remote(src, dst, send, recv, **where):
        return pltpu.make_async_remote_copy(
            src_ref=src, dst_ref=dst, send_sem=send, recv_sem=recv,
            device_id=where, device_id_type=MESH,
        )

    tab_copies = []
    for win in range(groups):
        first = win * window
        tab_copies.append(pltpu.make_async_copy(
            tables_ref.at[0, pl.ds(first, window)], tab.at[win, pl.ds(0, window)], tab_sem.at[2 * win]))
        tab_copies.append(pltpu.make_async_copy(
            tables_ref.at[0, pl.ds(first, HOT)], tab.at[win, pl.ds(window, HOT)], tab_sem.at[2 * win + 1]))
    for copy in tab_copies:
        copy.start()

    barrier = pltpu.get_barrier_semaphore()
    peers = [lax.rem(me + step, shards) for step in range(1, shards)]
    grp_peers = [lax.rem(grp + step, groups) for step in range(1, groups)]
    for peer in peers:
        pl.semaphore_signal(barrier, inc=1, device_id={"shard": peer}, device_id_type=MESH)
    for peer in grp_peers:
        pl.semaphore_signal(barrier, inc=1, device_id={"grp": peer}, device_id_type=MESH)
    looks[me] = lookups_ref[...]
    bottom_wide = bottom_ref[...].astype(jnp.float32)
    bottoms[me] = bottom_wide
    pl.semaphore_wait(barrier, len(peers) + len(grp_peers))

    sends = []
    for peer in peers:
        copy = remote(looks.at[me], looks.at[me], look_send.at[peer], look_recv.at[me], shard=peer)
        copy.start()
        sends.append(copy)
    far_chips = [lax.rem(chip + step, chips) for step in range(1, chips)]
    for peer in [other * 2 + core for other in far_chips] + [sib]:
        copy = remote(bottoms.at[me], bottoms.at[me], bot_send.at[peer], bot_recv.at[me], shard=peer)
        copy.start()
        sends.append(copy)

    preact_ref[...] = jnp.dot(bottom_ref[...], dense_ref[...], preferred_element_type=jnp.float32)

    for copy in tab_copies:
        copy.wait()
    flipped = []
    for win in range(groups):
        start = starts_ref[grp, me * groups + win]
        flipped.append(tab[win, pl.ds(start, HOT), :].T)
    hot_high, hot_low = split_two(jnp.concatenate(flipped, axis=1))
    hot_both = jnp.concatenate([hot_high, hot_low], axis=0)

    slot = lax.broadcasted_iota(jnp.int32, (hot_rows, batch), 0)
    wanted = slot + lax.div(slot, HOT) * (window - HOT) + me * (groups * window)

    def partial_sum(source):
        rows = looks[source]
        hits = jnp.zeros((hot_rows, batch), jnp.float32)
        for place in range(bag):
            hits = hits + jnp.where(rows[place:place + 1, :] == wanted, 1.0, 0.0)
        hits = hits.astype(jnp.bfloat16)
        counts[:, pl.ds(pl.multiple_of(source * batch, batch), batch)] = hits
        both = jnp.dot(hot_both, hits, preferred_element_type=jnp.float32)
        return both[:width] + both[width:]

    def look_wait(source):
        remote(looks.at[source], looks.at[source], look_send.at[source], look_recv.at[source],
               shard=source).wait_recv()

    for other in far_chips + [chip]:
        source = other * 2 + 1 - core
        look_wait(source)
        part_far[other] = partial_sum(source)
        copy = remote(part_far.at[other], from_sib.at[other], sib_send.at[other], sib_recv.at[other], shard=sib)
        copy.start()
        sends.append(copy)
    for other in far_chips:
        look_wait(other * 2 + core)
        part_own[other] = partial_sum(other * 2 + core)
    part_own[chip] = partial_sum(me)

    def sib_wait(other):
        remote(part_far.at[other], from_sib.at[other], sib_send.at[other], sib_recv.at[other],
               shard=sib).wait_recv()

    for other in far_chips:
        sib_wait(other)
        part_own[other] = part_own[other] + from_sib[other]
        copy = remote(part_own.at[other], arrived.at[chip], sum_send.at[other], sum_recv.at[chip],
                      shard=other * 2 + core)
        copy.start()
        sends.append(copy)

    def bottom_wait(source):
        remote(bottoms.at[source], bottoms.at[source], bot_send.at[source], bot_recv.at[source],
               shard=sib).wait_recv()

    for other in far_chips:
        source = other * 2 + core
        bottom_wait(source)
        copy = remote(bottoms.at[source], bottoms.at[source], bot_send.at[other * 2 + 1 - core],
                      bot_recv.at[source], shard=sib)
        copy.start()
        sends.append(copy)

    sib_wait(chip)
    pooled_flip = part_own[chip] + from_sib[chip]
    for other in far_chips:
        remote(part_own.at[other], arrived.at[other], sum_send.at[other], sum_recv.at[other],
               shard=other * 2 + core).wait_recv()
        pooled_flip = pooled_flip + arrived[other]
    pooled = pooled_flip.T
    dots = jnp.sum(bottom_wide * pooled, axis=1, keepdims=True)

    chunk = 256 if hidden % 256 == 0 else hidden
    lanes = 128 if chunk % 128 == 0 else chunk
    running = jnp.zeros((batch, lanes), jnp.float32)
    for first in range(0, hidden, chunk):
        cut = slice(first, first + chunk)
        weights = pairs_ref[0:1, cut]
        preact = preact_ref[:, cut] + dots * weights
        sig = jax.nn.sigmoid(preact)
        preact_ref[:, cut] = preact * sig
        pre_grad = cot_ref[:, cut] * sig * (1.0 + preact * (1.0 - sig))
        half_ref[:, cut] = pre_grad.astype(jnp.bfloat16)
        product = pre_grad * weights
        for lane in range(0, chunk, lanes):
            running = running + product[:, lane:lane + lanes]
    pair_col = jnp.sum(running, axis=1, keepdims=True)
    pair_row = jnp.broadcast_to(pair_col, (batch, 128)).T[0:8]
    pair_all[me] = pair_row
    for peer in peers:
        copy = remote(pair_all.at[me], pair_all.at[me], pair_send.at[peer], pair_recv.at[me], shard=peer)
        copy.start()
        sends.append(copy)

    act_ref[...] = preact_ref[...].astype(jnp.bfloat16)
    bottom_grad_ref[...] = lax.dot_general(
        half_ref[...], dense_ref[...], (((1,), (1,)), ((), ())), preferred_element_type=jnp.float32
    ) + pair_col * pooled

    for other in far_chips:
        bottom_wait(other * 2 + 1 - core)
    bottom_wait(sib)
    for peer in peers:
        remote(pair_all.at[peer], pair_all.at[peer], pair_send.at[peer], pair_recv.at[peer],
               shard=peer).wait_recv()
    for source in range(shards):
        column = jnp.broadcast_to(pair_all[source][0:1, :], (width, batch)).T
        high, low = split_two(bottoms[source] * column)
        weighted[source * batch:(source + 1) * batch, 0:width] = high
        weighted[source * batch:(source + 1) * batch, width:2 * width] = low
    per_dot = 4 if groups % 4 == 0 else 1
    for win in range(0, groups, per_dot):
        both = jnp.dot(counts[win * HOT:(win + per_dot) * HOT, :], weighted[...],
                       preferred_element_type=jnp.float32)
        summed = both[:, :width] + both[:, width:]
        for step in range(per_dot):
            grad_send[win + step] = summed[step * HOT:(step + 1) * HOT]
    for peer in grp_peers:
        copy = remote(grad_send.at[peer], grad_recv.at[grp], grp_send.at[peer], grp_recv.at[grp], grp=peer)
        copy.start()
        sends.append(copy)
    hot_out_ref[grp] = grad_send[grp]
    for peer in grp_peers:
        remote(grad_send.at[peer], grad_recv.at[peer], grp_send.at[peer], grp_recv.at[peer],
               grp=peer).wait_recv()
        hot_out_ref[peer] = grad_recv[peer]
    for copy in sends:
        copy.wait_send()


def place_kernel(groups, window, starts_ref, hot_ref, act_in, bottom_in, act_out, bottom_out, table_out,
                 spread, sem):
    me = lax.axis_index("shard")
    grp = lax.axis_index("grp")
    act_copy = pltpu.make_async_copy(act_in, act_out, sem.at[0])
    bottom_copy = pltpu.make_async_copy(bottom_in, bottom_out, sem.at[1])
    act_copy.start()
    bottom_copy.start()
    spread[...] = jnp.zeros_like(spread)
    for source in range(groups):
        start = starts_ref[source, me * groups + grp]
        spread[pl.ds(start, HOT), :] += hot_ref[source]
    spread[0:HOT, :] += spread[window:window + HOT, :]
    table_copy = pltpu.make_async_copy(spread.at[pl.ds(0, window)], table_out.at[0, 0], sem.at[2])
    table_copy.start()
    act_copy.wait()
    bottom_copy.wait()
    table_copy.wait()


def on_device(groups, shards, bottom_out, lookups, starts, tables, top_dense, top_pairs, cotangent):
    batch, width = bottom_out.shape
    hidden = cotangent.shape[1]
    bag = lookups.shape[2]
    window = tables.shape[1] // groups
    hot_rows = groups * HOT
    chips = shards // 2
    flipped = lookups[:, 0, :].T
    in_vmem = pl.BlockSpec(memory_space=VMEM)
    in_smem = pl.BlockSpec(memory_space=pltpu.SMEM)
    anywhere = pl.BlockSpec(memory_space=pl.ANY)
    f32, bf16 = jnp.float32, jnp.bfloat16
    blocks = VMEM((chips, width, batch), f32)
    act, bottom_grad, hot_grad = pl.pallas_call(
        functools.partial(exchange_kernel, groups, shards, window),
        out_shape=(
            jax.ShapeDtypeStruct((batch, hidden), bf16),
            jax.ShapeDtypeStruct((batch, width), f32),
            jax.ShapeDtypeStruct((groups, HOT, width), f32),
        ),
        in_specs=[in_smem, in_vmem, in_vmem, anywhere, in_vmem, in_vmem, in_vmem],
        out_specs=(in_vmem, in_vmem, in_vmem),
        scratch_shapes=[
            VMEM((groups, window + HOT, width), f32),
            VMEM((shards, bag, batch), jnp.int32),
            VMEM((shards, batch, width), f32),
            VMEM((hot_rows, shards * batch), bf16),
            blocks, blocks, blocks, blocks,
            VMEM((shards, 8, 128), f32),
            VMEM((shards * batch, 2 * width), bf16),
            VMEM((batch, hidden), f32),
            VMEM((batch, hidden), bf16),
            VMEM((groups, HOT, width), f32),
            VMEM((groups, HOT, width), f32),
            DMA((2 * groups,)),
            DMA((shards,)), DMA((shards,)), DMA((shards,)), DMA((shards,)),
            DMA((chips,)), DMA((chips,)), DMA((chips,)), DMA((chips,)),
            DMA((shards,)), DMA((shards,)), DMA((groups,)), DMA((groups,)),
        ],
        compiler_params=pltpu.CompilerParams(
            collective_id=0, has_side_effects=True, vmem_limit_bytes=48 * 1024 * 1024
        ),
    )(starts, flipped, bottom_out, tables, top_dense, top_pairs, cotangent)
    return pl.pallas_call(
        functools.partial(place_kernel, groups, window),
        out_shape=(
            jax.ShapeDtypeStruct((batch, hidden), bf16),
            jax.ShapeDtypeStruct((batch, width), f32),
            jax.ShapeDtypeStruct((1, 1, window, width), f32),
        ),
        in_specs=[in_smem, in_vmem, in_vmem, in_vmem],
        out_specs=(anywhere, anywhere, anywhere),
        scratch_shapes=[VMEM((window + HOT, width), f32), DMA((3,))],
        compiler_params=pltpu.CompilerParams(vmem_limit_bytes=16 * 1024 * 1024),
    )(starts, hot_grad, act, bottom_grad)


def solution(mesh):
    groups, shards = mesh.shape["grp"], mesh.shape["shard"]
    in_specs = (
        P(("grp", "shard"), None),
        P(("grp", "shard"), None, None),
        P(),
        P(None, "shard", None),
        P(),
        P(),
        P(("grp", "shard"), None),
    )
    out_specs = (
        P(("grp", "shard"), None),
        P(("grp", "shard"), None),
        P(None, "shard", "grp", None),
    )
    return jax.shard_map(
        functools.partial(on_device, groups, shards),
        mesh=mesh, in_specs=in_specs, out_specs=out_specs, check_vma=False,
    )
```

```python
import functools

import jax
import jax.numpy as jnp
from jax import lax
from jax.experimental import pallas as pl
from jax.experimental.pallas import tpu as pltpu
from jax.sharding import PartitionSpec as P

HOT = 64
VMEM_ALL = 67043328
MESH = pl.DeviceIdType.MESH
VMEM = pltpu.VMEM
DMA = pltpu.SemaphoreType.DMA


def split_two(value):
    high = value.astype(jnp.bfloat16)
    low = (value - high.astype(jnp.float32)).astype(jnp.bfloat16)
    return high, low


def exchange_kernel(
    groups, shards, window,
    starts_ref, lookups_ref, bottom_ref, tables_ref, dense_ref, pairs_ref, cot_ref,
    act_ref, bottom_grad_ref, hot_out_ref,
    starts, bottom, dense, pairs, cot,
    tab, looks, bottoms, counts, partial, from_sib, arrived, dots_all, pair_all,
    weighted, preact_ref, half_ref, act, bottom_grad, grad_send,
    load_sem, tab_sem, look_send, look_recv, bot_send, bot_recv, sib_send, sib_recv,
    sum_send, sum_recv, dots_send, dots_recv, pair_send, pair_recv, grp_send, grp_recv,
):
    bag, batch = lookups_ref.shape
    width = bottom_ref.shape[1]
    hidden = cot_ref.shape[1]
    chips = shards // 2
    hot_rows = groups * HOT
    me = lax.axis_index("shard")
    grp = lax.axis_index("grp")
    core = lax.rem(me, 2)
    chip = lax.div(me, 2)
    sib = chip * 2 + 1 - core

    def remote(src, dst, send, recv, **where):
        return pltpu.make_async_remote_copy(
            src_ref=src, dst_ref=dst, send_sem=send, recv_sem=recv,
            device_id=where, device_id_type=MESH,
        )

    barrier = pltpu.get_barrier_semaphore()
    peers = [lax.rem(me + step, shards) for step in range(1, shards)]
    grp_peers = [lax.rem(grp + step, groups) for step in range(1, groups)]
    for peer in peers:
        pl.semaphore_signal(barrier, inc=1, device_id={"shard": peer}, device_id_type=MESH)
    for peer in grp_peers:
        pl.semaphore_signal(barrier, inc=1, device_id={"grp": peer}, device_id_type=MESH)

    def load(src, dst, place):
        copy = pltpu.make_async_copy(src, dst, load_sem.at[place])
        copy.start()
        return copy

    bottom_load = load(bottom_ref, bottom, 0)
    look_load = load(lookups_ref, looks.at[me], 1)
    starts_load = load(starts_ref, starts, 2)
    dense_load = load(dense_ref, dense, 3)
    tab_copies = []
    for win in range(groups):
        first = win * window
        tab_copies.append(pltpu.make_async_copy(
            tables_ref.at[0, pl.ds(first, window)], tab.at[win, pl.ds(0, window)], tab_sem.at[2 * win]))
        tab_copies.append(pltpu.make_async_copy(
            tables_ref.at[0, pl.ds(first, HOT)], tab.at[win, pl.ds(window, HOT)], tab_sem.at[2 * win + 1]))
    for copy in tab_copies:
        copy.start()
    pairs_load = load(pairs_ref, pairs, 4)
    cot_load = load(cot_ref, cot, 5)

    bottom_load.wait()
    bottoms[me] = bottom[...].astype(jnp.float32).T
    look_load.wait()
    pl.semaphore_wait(barrier, len(peers) + len(grp_peers))

    sends = []

    def send(src, dst, send_sem, recv_sem, **where):
        copy = remote(src, dst, send_sem, recv_sem, **where)
        copy.start()
        sends.append(copy)

    far_chips = [lax.rem(chip + step, chips) for step in range(1, chips)]
    for peer in peers:
        send(looks.at[me], looks.at[me], look_send.at[peer], look_recv.at[me], shard=peer)
    for peer in [other * 2 + core for other in far_chips] + [sib]:
        send(bottoms.at[me], bottoms.at[me], bot_send.at[peer], bot_recv.at[me], shard=peer)

    dense_load.wait()
    preact_ref[...] = jnp.dot(bottom[...], dense[...], preferred_element_type=jnp.float32)

    starts_load.wait()
    for copy in tab_copies:
        copy.wait()
    flipped = []
    for win in range(groups):
        start = starts[grp, me * groups + win]
        flipped.append(tab[win, pl.ds(start, HOT), :].T)
    hot_high, hot_low = split_two(jnp.concatenate(flipped, axis=1))
    hot_both = jnp.concatenate([hot_high, hot_low], axis=0)

    slot = lax.broadcasted_iota(jnp.int32, (hot_rows, batch), 0)
    wanted = slot + lax.div(slot, HOT) * (window - HOT) + me * (groups * window)

    def pool(source):
        rows = looks[source]
        hits = jnp.zeros((hot_rows, batch), jnp.float32)
        for place in range(bag):
            hits = hits + jnp.where(rows[place:place + 1, :] == wanted, 1.0, 0.0)
        hits = hits.astype(jnp.bfloat16)
        counts[:, pl.ds(pl.multiple_of(source * batch, batch), batch)] = hits
        both = jnp.dot(hot_both, hits, preferred_element_type=jnp.float32)
        partial[source] = both[:width] + both[width:]

    def look_wait(source):
        remote(looks.at[source], looks.at[source], look_send.at[source], look_recv.at[source],
               shard=source).wait_recv()

    pool(me)
    for source in [sib] + [other * 2 + 1 - core for other in far_chips]:
        look_wait(source)
        pool(source)
        other = lax.div(source, 2)
        send(partial.at[source], from_sib.at[other], sib_send.at[other], sib_recv.at[other], shard=sib)
    for other in far_chips:
        look_wait(other * 2 + core)
        pool(other * 2 + core)

    def dot_row(source):
        return jnp.sum(partial[source] * bottoms[source], axis=0, keepdims=True)

    def bottom_wait(source):
        remote(bottoms.at[source], bottoms.at[source], bot_send.at[source], bot_recv.at[source],
               shard=sib).wait_recv()

    def dot_send(source):
        dots_all[source] = dot_row(source)
        send(dots_all.at[source], pair_all.at[0, me], dots_send.at[source], dots_recv.at[me], shard=source)

    bottom_wait(sib)
    dot_send(sib)
    near_first = []
    for step in range(1, chips // 2 + 1):
        near_first.append(lax.rem(chip + step, chips))
        if step != chips - step:
            near_first.append(lax.rem(chip + chips - step, chips))
    for other in near_first:
        source = other * 2 + core
        bottom_wait(source)
        send(bottoms.at[source], bottoms.at[source], bot_send.at[other * 2 + 1 - core],
             bot_recv.at[source], shard=sib)
        dot_send(source)
    for other in near_first:
        source = other * 2 + 1 - core
        bottom_wait(source)
        dot_send(source)
    dots = dot_row(me)

    def sib_wait(other):
        remote(from_sib.at[other], from_sib.at[other], sib_send.at[other], sib_recv.at[other],
               shard=sib).wait_recv()

    for other in far_chips:
        sib_wait(other)
        from_sib[other] = from_sib[other] + partial[other * 2 + core]
        send(from_sib.at[other], arrived.at[chip], sum_send.at[other], sum_recv.at[chip],
             shard=other * 2 + core)

    for peer in peers:
        remote(dots_all.at[peer], pair_all.at[0, peer], dots_send.at[peer], dots_recv.at[peer],
               shard=peer).wait_recv()
        dots = dots + pair_all[0, peer]
    dots_col = jnp.broadcast_to(dots, (batch, batch)).T[:, 0:1]

    pairs_load.wait()
    cot_load.wait()
    chunk = 256 if hidden % 256 == 0 else hidden
    lanes = 128 if chunk % 128 == 0 else chunk
    running = jnp.zeros((batch, lanes), jnp.float32)
    for first in range(0, hidden, chunk):
        cut = slice(first, first + chunk)
        weights = pairs[0:1, cut]
        preact = preact_ref[:, cut] + dots_col * weights
        sig = jax.nn.sigmoid(preact)
        preact_ref[:, cut] = preact * sig
        pre_grad = cot[:, cut] * sig * (1.0 + preact * (1.0 - sig))
        half_ref[:, cut] = pre_grad.astype(jnp.bfloat16)
        product = pre_grad * weights
        for lane in range(0, chunk, lanes):
            running = running + product[:, lane:lane + lanes]
    pair_col = jnp.sum(running, axis=1, keepdims=True)
    pair_all[1, me] = jnp.broadcast_to(pair_col, (batch, batch)).T[0:1]
    for peer in peers:
        send(pair_all.at[1, me], pair_all.at[1, me], pair_send.at[peer], pair_recv.at[me], shard=peer)

    act[...] = preact_ref[...].astype(jnp.bfloat16)
    act_store = load(act, act_ref, 6)
    bottom_dense = lax.dot_general(
        half_ref[...], dense[...], (((1,), (1,)), ((), ())), preferred_element_type=jnp.float32
    )

    def weigh(source):
        high, low = split_two(bottoms[source] * pair_all[1, source])
        where = pl.ds(pl.multiple_of(source * batch, batch), batch)
        weighted[0:width, where] = high
        weighted[width:2 * width, where] = low

    weigh(me)
    for peer in peers:
        remote(pair_all.at[1, peer], pair_all.at[1, peer], pair_send.at[peer], pair_recv.at[peer],
               shard=peer).wait_recv()
        weigh(peer)
    per_dot = 4 if groups % 4 == 0 else 1
    for win in range(0, groups, per_dot):
        both = lax.dot_general(
            counts[win * HOT:(win + per_dot) * HOT, :], weighted[...],
            (((1,), (1,)), ((), ())), preferred_element_type=jnp.float32)
        summed = both[:, :width] + both[:, width:]
        for step in range(per_dot):
            grad_send[win + step] = summed[step * HOT:(step + 1) * HOT]
    for peer in grp_peers:
        send(grad_send.at[peer], hot_out_ref.at[grp], grp_send.at[peer], grp_recv.at[grp], grp=peer)
    own_store = load(grad_send.at[grp], hot_out_ref.at[grp], 7)

    sib_wait(chip)
    pooled = partial[me] + from_sib[chip]
    for other in far_chips:
        remote(from_sib.at[other], arrived.at[other], sum_send.at[other], sum_recv.at[other],
               shard=other * 2 + core).wait_recv()
        pooled = pooled + arrived[other]
    bottom_grad[...] = bottom_dense + (pooled * pair_all[1, me]).T
    bottom_store = load(bottom_grad, bottom_grad_ref, 8)
    for peer in grp_peers:
        remote(grad_send.at[peer], hot_out_ref.at[peer], grp_send.at[peer], grp_recv.at[peer],
               grp=peer).wait_recv()
    act_store.wait()
    own_store.wait()
    bottom_store.wait()
    for copy in sends:
        copy.wait_send()


def place_kernel(groups, window, starts_ref, hot_ref, act_in, bottom_in, act_out, bottom_out, table_out,
                 spread, starts, hot, act, bottom, sem):
    me = lax.axis_index("shard")
    grp = lax.axis_index("grp")

    def copy(src, dst, place):
        started = pltpu.make_async_copy(src, dst, sem.at[place])
        started.start()
        return started

    hot_load = copy(hot_ref, hot, 0)
    starts_load = copy(starts_ref, starts, 1)
    act_load = copy(act_in, act, 2)
    bottom_load = copy(bottom_in, bottom, 3)
    spread[...] = jnp.zeros_like(spread)
    starts_load.wait()
    hot_load.wait()
    for source in range(groups):
        start = starts[source, me * groups + grp]
        spread[pl.ds(start, HOT), :] += hot[source]
    spread[0:HOT, :] += spread[window:window + HOT, :]
    table_store = copy(spread.at[pl.ds(0, window)], table_out.at[0, 0], 4)
    act_load.wait()
    act_store = copy(act, act_out, 5)
    bottom_load.wait()
    bottom_store = copy(bottom, bottom_out, 6)
    act_store.wait()
    bottom_store.wait()
    table_store.wait()


def on_device(groups, shards, bottom_out, lookups, starts, tables, top_dense, top_pairs, cotangent):
    batch, width = bottom_out.shape
    hidden = cotangent.shape[1]
    bag = lookups.shape[2]
    window = tables.shape[1] // groups
    hot_rows = groups * HOT
    chips = shards // 2
    flipped = lookups[:, 0, :].T
    in_hbm = pl.BlockSpec(memory_space=pltpu.HBM)
    f32, bf16 = jnp.float32, jnp.bfloat16
    blocks = VMEM((chips, width, batch), f32)
    act, bottom_grad, hot_grad = pl.pallas_call(
        functools.partial(exchange_kernel, groups, shards, window),
        out_shape=(
            jax.ShapeDtypeStruct((batch, hidden), bf16),
            jax.ShapeDtypeStruct((batch, width), f32),
            jax.ShapeDtypeStruct((groups, HOT, width), f32),
        ),
        in_specs=[in_hbm] * 7,
        out_specs=(in_hbm, in_hbm, in_hbm),
        scratch_shapes=[
            pltpu.SMEM(starts.shape, jnp.int32),
            VMEM((batch, width), bf16),
            VMEM((width, hidden), bf16),
            VMEM((1, hidden), f32),
            VMEM((batch, hidden), f32),
            VMEM((groups, window + HOT, width), f32),
            VMEM((shards, bag, batch), jnp.int32),
            VMEM((shards, width, batch), f32),
            VMEM((hot_rows, shards * batch), bf16),
            VMEM((shards, width, batch), f32), blocks, blocks,
            VMEM((shards, 1, batch), f32),
            VMEM((2, shards, 1, batch), f32),
            VMEM((2 * width, shards * batch), bf16),
            VMEM((batch, hidden), f32),
            VMEM((batch, hidden), bf16),
            VMEM((batch, hidden), bf16),
            VMEM((batch, width), f32),
            VMEM((groups, HOT, width), f32),
            DMA((9,)), DMA((2 * groups,)),
            DMA((shards,)), DMA((shards,)), DMA((shards,)), DMA((shards,)),
            DMA((chips,)), DMA((chips,)), DMA((chips,)), DMA((chips,)),
            DMA((shards,)), DMA((shards,)), DMA((shards,)), DMA((shards,)),
            DMA((groups,)), DMA((groups,)),
        ],
        compiler_params=pltpu.CompilerParams(
            collective_id=0, has_side_effects=True, vmem_limit_bytes=VMEM_ALL
        ),
    )(starts, flipped, bottom_out, tables, top_dense, top_pairs, cotangent)
    return pl.pallas_call(
        functools.partial(place_kernel, groups, window),
        out_shape=(
            jax.ShapeDtypeStruct((batch, hidden), bf16),
            jax.ShapeDtypeStruct((batch, width), f32),
            jax.ShapeDtypeStruct((1, 1, window, width), f32),
        ),
        in_specs=[in_hbm] * 4,
        out_specs=(in_hbm, in_hbm, in_hbm),
        scratch_shapes=[
            VMEM((window + HOT, width), f32),
            pltpu.SMEM(starts.shape, jnp.int32),
            VMEM((groups, HOT, width), f32),
            VMEM((batch, hidden), bf16),
            VMEM((batch, width), f32),
            DMA((7,)),
        ],
        compiler_params=pltpu.CompilerParams(vmem_limit_bytes=VMEM_ALL),
    )(starts, hot_grad, act, bottom_grad)


def solution(mesh):
    groups, shards = mesh.shape["grp"], mesh.shape["shard"]
    in_specs = (
        P(("grp", "shard"), None),
        P(("grp", "shard"), None, None),
        P(),
        P(None, "shard", None),
        P(),
        P(),
        P(("grp", "shard"), None),
    )
    out_specs = (
        P(("grp", "shard"), None),
        P(("grp", "shard"), None),
        P(None, "shard", "grp", None),
    )
    return jax.shard_map(
        functools.partial(on_device, groups, shards),
        mesh=mesh, in_specs=in_specs, out_specs=out_specs, check_vma=False,
    )
```

```python
import functools

import jax
import jax.numpy as jnp
from jax import lax
from jax.experimental import pallas as pl
from jax.experimental.pallas import tpu as pltpu
from jax.sharding import PartitionSpec as P

HOT = 64
VMEM_ALL = 67043328
MESH = pl.DeviceIdType.MESH
VMEM = pltpu.VMEM
DMA = pltpu.SemaphoreType.DMA


def split_two(value):
    high = value.astype(jnp.bfloat16)
    low = (value - high.astype(jnp.float32)).astype(jnp.bfloat16)
    return high, low


def exchange_kernel(
    groups, shards, window,
    starts_ref, lookups_ref, bottom_ref, tables_ref, dense_ref, pairs_ref, cot_ref,
    act_ref, bottom_grad_ref, hot_out_ref,
    starts, bottom, dense, pairs, cot,
    tab, looks, bottoms, counts, partial, from_sib, arrived, dots_all, pair_all,
    weighted, preact_ref, half_ref, act, bottom_grad, grad_send,
    load_sem, tab_sem, look_send, look_recv, bot_send, bot_recv, sib_send, sib_recv,
    sum_send, sum_recv, dots_send, dots_recv, pair_send, pair_recv, grp_send, grp_recv,
):
    bag, batch = lookups_ref.shape
    width = bottom_ref.shape[1]
    hidden = cot_ref.shape[1]
    chips = shards // 2
    hot_rows = groups * HOT
    me = lax.axis_index("shard")
    grp = lax.axis_index("grp")
    core = lax.rem(me, 2)
    chip = lax.div(me, 2)
    sib = chip * 2 + 1 - core

    def remote(src, dst, send, recv, **where):
        return pltpu.make_async_remote_copy(
            src_ref=src, dst_ref=dst, send_sem=send, recv_sem=recv,
            device_id=where, device_id_type=MESH,
        )

    barrier = pltpu.get_barrier_semaphore()
    peers = [lax.rem(me + step, shards) for step in range(1, shards)]
    grp_peers = [lax.rem(grp + step, groups) for step in range(1, groups)]
    for peer in peers:
        pl.semaphore_signal(barrier, inc=1, device_id={"shard": peer}, device_id_type=MESH)
    for peer in grp_peers:
        pl.semaphore_signal(barrier, inc=1, device_id={"grp": peer}, device_id_type=MESH)

    def load(src, dst, place):
        copy = pltpu.make_async_copy(src, dst, load_sem.at[place])
        copy.start()
        return copy

    bottom_load = load(bottom_ref, bottom, 0)
    look_load = load(lookups_ref, looks.at[me], 1)
    starts_load = load(starts_ref, starts, 2)
    dense_load = load(dense_ref, dense, 3)
    tab_copies = []
    for win in range(groups):
        first = win * window
        tab_copies.append(pltpu.make_async_copy(
            tables_ref.at[0, pl.ds(first, window)], tab.at[win, pl.ds(0, window)], tab_sem.at[2 * win]))
        tab_copies.append(pltpu.make_async_copy(
            tables_ref.at[0, pl.ds(first, HOT)], tab.at[win, pl.ds(window, HOT)], tab_sem.at[2 * win + 1]))
    for copy in tab_copies:
        copy.start()
    pairs_load = load(pairs_ref, pairs, 4)
    cot_load = load(cot_ref, cot, 5)

    bottom_load.wait()
    bottoms[me] = bottom[...].astype(jnp.float32).T
    look_load.wait()
    pl.semaphore_wait(barrier, len(peers) + len(grp_peers))

    sends = []

    def send(src, dst, send_sem, recv_sem, **where):
        copy = remote(src, dst, send_sem, recv_sem, **where)
        copy.start()
        sends.append(copy)

    far_chips = [lax.rem(chip + step, chips) for step in range(1, chips)]
    for peer in peers:
        send(looks.at[me], looks.at[me], look_send.at[peer], look_recv.at[me], shard=peer)
    for peer in [other * 2 + core for other in far_chips] + [sib]:
        send(bottoms.at[me], bottoms.at[me], bot_send.at[peer], bot_recv.at[me], shard=peer)

    dense_load.wait()
    preact_ref[...] = jnp.dot(bottom[...], dense[...], preferred_element_type=jnp.float32)

    starts_load.wait()
    for copy in tab_copies:
        copy.wait()
    flipped = []
    for win in range(groups):
        start = starts[grp, me * groups + win]
        flipped.append(tab[win, pl.ds(start, HOT), :].T)
    hot_high, hot_low = split_two(jnp.concatenate(flipped, axis=1))
    hot_both = jnp.concatenate([hot_high, hot_low], axis=0)

    slot = lax.broadcasted_iota(jnp.int32, (hot_rows, batch), 0)
    wanted = slot + lax.div(slot, HOT) * (window - HOT) + me * (groups * window)

    def pool(source):
        rows = looks[source]
        hits = jnp.zeros((hot_rows, batch), jnp.float32)
        for place in range(bag):
            hits = hits + jnp.where(rows[place:place + 1, :] == wanted, 1.0, 0.0)
        hits = hits.astype(jnp.bfloat16)
        counts[:, pl.ds(pl.multiple_of(source * batch, batch), batch)] = hits
        both = jnp.dot(hot_both, hits, preferred_element_type=jnp.float32)
        partial[source] = both[:width] + both[width:]

    def look_wait(source):
        remote(looks.at[source], looks.at[source], look_send.at[source], look_recv.at[source],
               shard=source).wait_recv()

    pool(me)
    for source in [sib] + [other * 2 + 1 - core for other in far_chips]:
        look_wait(source)
        pool(source)
        other = lax.div(source, 2)
        send(partial.at[source], from_sib.at[other], sib_send.at[other], sib_recv.at[other], shard=sib)
    for other in far_chips:
        look_wait(other * 2 + core)
        pool(other * 2 + core)

    def dot_row(source):
        return jnp.sum(partial[source] * bottoms[source], axis=0, keepdims=True)

    def bottom_wait(source):
        remote(bottoms.at[source], bottoms.at[source], bot_send.at[source], bot_recv.at[source],
               shard=sib).wait_recv()

    def dot_send(source):
        dots_all[source] = dot_row(source)
        send(dots_all.at[source], pair_all.at[0, me], dots_send.at[source], dots_recv.at[me], shard=source)

    bottom_wait(sib)
    dot_send(sib)
    near_first = []
    for step in range(1, chips // 2 + 1):
        near_first.append(lax.rem(chip + step, chips))
        if step != chips - step:
            near_first.append(lax.rem(chip + chips - step, chips))
    for other in near_first:
        source = other * 2 + core
        bottom_wait(source)
        send(bottoms.at[source], bottoms.at[source], bot_send.at[other * 2 + 1 - core],
             bot_recv.at[source], shard=sib)
        dot_send(source)
    for other in near_first:
        source = other * 2 + 1 - core
        bottom_wait(source)
        dot_send(source)
    dots = dot_row(me)

    def sib_wait(other):
        remote(from_sib.at[other], from_sib.at[other], sib_send.at[other], sib_recv.at[other],
               shard=sib).wait_recv()

    for other in far_chips:
        sib_wait(other)
        from_sib[other] = from_sib[other] + partial[other * 2 + core]
        send(from_sib.at[other], arrived.at[chip], sum_send.at[other], sum_recv.at[chip],
             shard=other * 2 + core)

    for peer in peers:
        remote(dots_all.at[peer], pair_all.at[0, peer], dots_send.at[peer], dots_recv.at[peer],
               shard=peer).wait_recv()
        dots = dots + pair_all[0, peer]
    dots_tile = jnp.broadcast_to(dots, (batch, batch)).T

    pairs_load.wait()
    cot_load.wait()
    running = jnp.zeros((batch, batch), jnp.float32)
    for first in range(0, hidden, batch):
        cut = slice(first, first + batch)
        weights = pairs[0:1, cut]
        preact = preact_ref[:, cut] + dots_tile * weights
        sig = 0.5 + 0.5 * jnp.tanh(0.5 * preact)
        act[:, cut] = (preact * sig).astype(jnp.bfloat16)
        pre_grad = cot[:, cut] * sig * (1.0 + preact * (1.0 - sig))
        half_ref[:, cut] = pre_grad.astype(jnp.bfloat16)
        running = running + pre_grad * weights
    pair_all[1, me] = jnp.sum(running.T, axis=0, keepdims=True)
    for peer in peers:
        send(pair_all.at[1, me], pair_all.at[1, me], pair_send.at[peer], pair_recv.at[me], shard=peer)

    act_store = load(act, act_ref, 6)
    bottom_dense = lax.dot_general(
        half_ref[...], dense[...], (((1,), (1,)), ((), ())), preferred_element_type=jnp.float32
    )

    def weigh(source):
        high, low = split_two(bottoms[source] * pair_all[1, source])
        where = pl.ds(pl.multiple_of(source * batch, batch), batch)
        weighted[0:width, where] = high
        weighted[width:2 * width, where] = low

    def pair_wait(source):
        remote(pair_all.at[1, source], pair_all.at[1, source], pair_send.at[source], pair_recv.at[source],
               shard=sib).wait_recv()

    weigh(me)
    for other in [chip] + near_first:
        if other is not chip:
            pair_wait(other * 2 + core)
            weigh(other * 2 + core)
        pair_wait(other * 2 + 1 - core)
        weigh(other * 2 + 1 - core)
        where = pl.ds(pl.multiple_of(other * 2 * batch, batch), 2 * batch)
        both = lax.dot_general(counts[:, where], weighted[:, where], (((1,), (1,)), ((), ())),
                               preferred_element_type=jnp.float32)
        summed = (both[:, :width] + both[:, width:]).reshape(groups, HOT, width)
        if other is chip:
            grad_send[...] = summed
        else:
            grad_send[...] = grad_send[...] + summed
    for peer in grp_peers:
        send(grad_send.at[peer], hot_out_ref.at[grp], grp_send.at[peer], grp_recv.at[grp], grp=peer)
    own_store = load(grad_send.at[grp], hot_out_ref.at[grp], 7)

    sib_wait(chip)
    pooled = partial[me] + from_sib[chip]
    for other in far_chips:
        remote(from_sib.at[other], arrived.at[other], sum_send.at[other], sum_recv.at[other],
               shard=other * 2 + core).wait_recv()
        pooled = pooled + arrived[other]
    bottom_grad[...] = bottom_dense + (pooled * pair_all[1, me]).T
    bottom_store = load(bottom_grad, bottom_grad_ref, 8)
    for peer in grp_peers:
        remote(grad_send.at[peer], hot_out_ref.at[peer], grp_send.at[peer], grp_recv.at[peer],
               grp=peer).wait_recv()
    act_store.wait()
    own_store.wait()
    bottom_store.wait()
    for copy in sends:
        copy.wait_send()


def place_kernel(groups, window, starts_ref, hot_ref, act_in, bottom_in, act_out, bottom_out, table_out,
                 spread, starts, hot, act, bottom, sem):
    me = lax.axis_index("shard")
    grp = lax.axis_index("grp")

    def copy(src, dst, place):
        started = pltpu.make_async_copy(src, dst, sem.at[place])
        started.start()
        return started

    hot_load = copy(hot_ref, hot, 0)
    starts_load = copy(starts_ref, starts, 1)
    act_load = copy(act_in, act, 2)
    bottom_load = copy(bottom_in, bottom, 3)
    spread[...] = jnp.zeros_like(spread)
    starts_load.wait()
    hot_load.wait()
    for source in range(groups):
        start = starts[source, me * groups + grp]
        spread[pl.ds(start, HOT), :] += hot[source]
    spread[0:HOT, :] += spread[window:window + HOT, :]
    table_store = copy(spread.at[pl.ds(0, window)], table_out.at[0, 0], 4)
    act_load.wait()
    act_store = copy(act, act_out, 5)
    bottom_load.wait()
    bottom_store = copy(bottom, bottom_out, 6)
    act_store.wait()
    bottom_store.wait()
    table_store.wait()


def on_device(groups, shards, bottom_out, lookups, starts, tables, top_dense, top_pairs, cotangent):
    batch, width = bottom_out.shape
    hidden = cotangent.shape[1]
    bag = lookups.shape[2]
    window = tables.shape[1] // groups
    hot_rows = groups * HOT
    chips = shards // 2
    flipped = lookups[:, 0, :].T
    in_hbm = pl.BlockSpec(memory_space=pltpu.HBM)
    f32, bf16 = jnp.float32, jnp.bfloat16
    blocks = VMEM((chips, width, batch), f32)
    act, bottom_grad, hot_grad = pl.pallas_call(
        functools.partial(exchange_kernel, groups, shards, window),
        out_shape=(
            jax.ShapeDtypeStruct((batch, hidden), bf16),
            jax.ShapeDtypeStruct((batch, width), f32),
            jax.ShapeDtypeStruct((groups, HOT, width), f32),
        ),
        in_specs=[in_hbm] * 7,
        out_specs=(in_hbm, in_hbm, in_hbm),
        scratch_shapes=[
            pltpu.SMEM(starts.shape, jnp.int32),
            VMEM((batch, width), bf16),
            VMEM((width, hidden), bf16),
            VMEM((1, hidden), f32),
            VMEM((batch, hidden), f32),
            VMEM((groups, window + HOT, width), f32),
            VMEM((shards, bag, batch), jnp.int32),
            VMEM((shards, width, batch), f32),
            VMEM((hot_rows, shards * batch), bf16),
            VMEM((shards, width, batch), f32), blocks, blocks,
            VMEM((shards, 1, batch), f32),
            VMEM((2, shards, 1, batch), f32),
            VMEM((2 * width, shards * batch), bf16),
            VMEM((batch, hidden), f32),
            VMEM((batch, hidden), bf16),
            VMEM((batch, hidden), bf16),
            VMEM((batch, width), f32),
            VMEM((groups, HOT, width), f32),
            DMA((9,)), DMA((2 * groups,)),
            DMA((shards,)), DMA((shards,)), DMA((shards,)), DMA((shards,)),
            DMA((chips,)), DMA((chips,)), DMA((chips,)), DMA((chips,)),
            DMA((shards,)), DMA((shards,)), DMA((shards,)), DMA((shards,)),
            DMA((groups,)), DMA((groups,)),
        ],
        compiler_params=pltpu.CompilerParams(
            collective_id=0, has_side_effects=True, vmem_limit_bytes=VMEM_ALL
        ),
    )(starts, flipped, bottom_out, tables, top_dense, top_pairs, cotangent)
    return pl.pallas_call(
        functools.partial(place_kernel, groups, window),
        out_shape=(
            jax.ShapeDtypeStruct((batch, hidden), bf16),
            jax.ShapeDtypeStruct((batch, width), f32),
            jax.ShapeDtypeStruct((1, 1, window, width), f32),
        ),
        in_specs=[in_hbm] * 4,
        out_specs=(in_hbm, in_hbm, in_hbm),
        scratch_shapes=[
            VMEM((window + HOT, width), f32),
            pltpu.SMEM(starts.shape, jnp.int32),
            VMEM((groups, HOT, width), f32),
            VMEM((batch, hidden), bf16),
            VMEM((batch, width), f32),
            DMA((7,)),
        ],
        compiler_params=pltpu.CompilerParams(vmem_limit_bytes=VMEM_ALL),
    )(starts, hot_grad, act, bottom_grad)


def solution(mesh):
    groups, shards = mesh.shape["grp"], mesh.shape["shard"]
    in_specs = (
        P(("grp", "shard"), None),
        P(("grp", "shard"), None, None),
        P(),
        P(None, "shard", None),
        P(),
        P(),
        P(("grp", "shard"), None),
    )
    out_specs = (
        P(("grp", "shard"), None),
        P(("grp", "shard"), None),
        P(None, "shard", "grp", None),
    )
    return jax.shard_map(
        functools.partial(on_device, groups, shards),
        mesh=mesh, in_specs=in_specs, out_specs=out_specs, check_vma=False,
    )
```
